32 devices in a mesh: groups: 2 (over y), ctx: 4 (over z), wt: 2 (over x), sub: 2 (over core).
Axes of the slice: x: 2, y: 2, z: 4, core: 2. Of those that a mesh axis runs over, the one named last changes fastest.
Arguments:
- queries: bfloat16 [16, 32, 128, 576], P(('groups', 'ctx'), None, ('wt', 'sub')), parts along dimension 0, may hold values from -80 to 80
- selection: int32 [16, 4, 2], P(('groups', 'ctx')), parts along dimension 0, may hold values from -1 to 15, as said below
- latent_cache: bfloat16 [128, 64, 576], P(('groups', 'ctx')), parts along dimension 0, may hold values from -8 to 8
- value_up: bfloat16 [128, 512, 128], P(None, ('wt', 'sub')), may hold values from -1 to 1
Outputs:
- attended: bfloat16 [16, 32, 128, 128], P(('groups', 'ctx'), None, ('wt', 'sub')), parts along dimension 0
The draws below stay inside these ranges and needn't reach their ends.
There are 2 independent parts, one for each index of `groups`. The reference program is written for one: setup_inputs(seed, part) draws one part's arguments, and reference() takes and returns one part's arrays. A program takes and returns all parts, laid end to end along the dimension named above; an argument that names none is the same for every part. Nothing has to cross between parts.
Inputs may be any that keep to these rules, and one draw needn't show every extreme that they name: `selection`: entry [c, o, s] is the number of a block among the 16 of owner o, or -1 for an empty slot; in an owner's slots live entries come first and differ. Each query block has 4 live entries in all, and in every query block some owner fills all 2 slots.
All inputs are finite; a program needn't handle non-finite values.
Results may differ from the reference program's by a relative error of at most 0.008.
Values may be sent and summed in bfloat16 or wider, within the bound.
A program may use at most 128 MiB of HBM per device.

```python
import jax
import jax.numpy as jnp
from jax import lax

HEADS = 128
LAT = 512
ROPE = 64
NOPE = 128
VDIM = 128
BLK = 64
QC = 32
BLK_OWN = 16
BLOCKS = 64
SPAN_ALL = 8
N_CTX = 4


def build_all(key):
    key_sel = jax.random.fold_in(key, 101)
    key_rank = jax.random.fold_in(key, 202)
    key_cache = jax.random.fold_in(key, 303)
    key_query = jax.random.fold_in(key, 404)
    rankings = jax.vmap(lambda k: jax.random.permutation(k, BLK_OWN))(jax.random.split(key_rank, N_CTX))

    def one_span(span_key):
        first, second, third, fourth = jax.random.split(span_key, 4)
        order = jax.random.permutation(first, N_CTX)
        hottest = jax.random.randint(second, (), 1, N_CTX // 4 + 1)
        position = jnp.zeros((N_CTX,), jnp.int32).at[order].set(jnp.arange(N_CTX, dtype=jnp.int32))
        loads = jnp.where(position < hottest, 2, jnp.where(position < 2 * hottest, 0, 1))
        picks = jnp.min(jax.random.randint(third, (4, N_CTX), 0, BLK_OWN), axis=0)
        jumps = jax.random.randint(fourth, (N_CTX,), 0, BLK_OWN - 1)
        owner_rows = jnp.arange(N_CTX)
        lead = rankings[owner_rows, picks]
        other = rankings[owner_rows, (picks + 1 + jumps) % BLK_OWN]
        slot_zero = jnp.where(loads >= 1, lead, -1)
        slot_one = jnp.where(loads >= 2, other, -1)
        chosen = jnp.stack([slot_zero, slot_one], axis=1).astype(jnp.int32)
        target = (order[0] * BLK_OWN + lead[order[0]]).astype(jnp.int32)
        return (chosen, target)
    selection, targets = jax.vmap(one_span)(jax.random.split(key_sel, SPAN_ALL))
    cache = jnp.clip(jax.random.normal(key_cache, (BLOCKS, BLK, LAT + ROPE), jnp.float32), -6.0, 6.0)
    query = jnp.clip(1.2 * jax.random.normal(key_query, (SPAN_ALL, QC, HEADS, LAT + ROPE), jnp.float32), -7.2, 7.2)
    return (selection, cache, query)


def draw_queries(key, part):
    selection, cache, query = build_all(key)
    return query.astype(jnp.bfloat16)


def draw_selection(key, part):
    selection, cache, query = build_all(key)
    return selection


def draw_latent_cache(key, part):
    selection, cache, query = build_all(key)
    return cache.astype(jnp.bfloat16)


def block_levels(stream_key, dims, shards, low, high):
    loudness, own = 1.0, jax.random.fold_in(stream_key, 6)
    for axis_at, blocks in shards:
        steps = jnp.exp(jax.random.uniform(jax.random.fold_in(own, axis_at), (blocks,), jnp.float32, low / len(shards), high / len(shards)))
        loudness = loudness * jnp.repeat(steps, dims[axis_at] // blocks).reshape([-1 if axis == axis_at else 1 for axis in range(len(dims))])
    return loudness


def noise(rng, dims, width, most, shards=(), kind=jnp.bfloat16):
    entries = width * jax.random.normal(rng, dims, jnp.float32)
    if shards:
        entries = entries * block_levels(rng, dims, shards, -0.22, 0.18)
    return jnp.clip(entries, -most, most).astype(kind)


def setup_inputs(seed: int = 0, part: int = 0) -> dict:
    seeds = jax.random.split(jax.random.key(seed), 5)
    part_splits = jax.random.split(jax.random.fold_in(seeds[4], part), 5)
    queries = draw_queries(jax.random.fold_in(jax.random.fold_in(seeds[4], part), 71), part)
    selection = draw_selection(jax.random.fold_in(jax.random.fold_in(seeds[4], part), 71), part)
    latent_cache = draw_latent_cache(jax.random.fold_in(jax.random.fold_in(seeds[4], part), 71), part)
    value_up = noise(seeds[3], (HEADS, LAT, VDIM), (LAT // 16) ** -0.5, 1.0, ((1, 4),))
    return dict(queries=queries, selection=selection, latent_cache=latent_cache, value_up=value_up)


def one_block(latent_cache, value_up, query, chosen):
    owner_base = (jnp.arange(N_CTX, dtype=jnp.int32) * BLK_OWN)[:, None]
    numbers = (owner_base + jnp.clip(chosen, 0, BLK_OWN - 1)).astype(jnp.int32)
    keys = latent_cache[numbers.reshape(-1)].reshape(-1, LAT + ROPE)
    live = jnp.repeat((chosen >= 0).reshape(-1), BLK)
    rows = query.reshape(-1, LAT + ROPE)
    scores = jnp.einsum("rd,kd->rk", rows, keys, preferred_element_type=jnp.float32)
    scores = scores * jnp.float32((NOPE + ROPE) ** -0.5)
    scores = jnp.where(live[None, :], scores, -jnp.inf)
    expo = jnp.exp(scores - jnp.max(scores, axis=1, keepdims=True))
    totals = jnp.sum(expo, axis=1, keepdims=True)
    weights = expo.astype(jnp.bfloat16)
    latent = (jnp.dot(weights, keys[:, :LAT], preferred_element_type=jnp.float32) / totals).astype(jnp.bfloat16)
    latent = latent.reshape(QC, HEADS, LAT)
    out = jnp.einsum("qhl,hlv->qhv", latent.astype(jnp.float32), value_up.astype(jnp.float32))
    return out.astype(jnp.bfloat16)


def reference(queries, selection, latent_cache, value_up):
    def step(pair):
        return one_block(latent_cache, value_up, pair[0], pair[1])
    return lax.map(step, (queries, selection))
```

```python
import functools

import jax
import jax.numpy as jnp
from jax import lax
from jax.experimental import pallas as pl
from jax.experimental.pallas import tpu as pltpu
from jax.sharding import PartitionSpec as P

LAT = 512
ROPE = 64
NOPE = 128
MESH = pl.DeviceIdType.MESH


def kernel(
    dims, sel_hbm, q_hbm, cache_hbm, up_hbm, res_v,
    q_v, cache_v, up_v, sel_sm, sel_in, sel_far, send_v, keys_v, lat_v, *rest,
):
    (G, C, W, S, spans, per_span, hh, slots, blk, width, R, V, stride, A, Y, Z) = dims
    kbufs = rest[:spans]
    (loc_sem, sel_snd, sel_rcv, sel_loc, x_snd, x_rcv, s_snd, s_rcv, y_snd, y_rcv,
     k_snd, k_rcv, f_snd, f_rcv, z_snd, z_rcv) = rest[spans:]
    half = slots // S
    RX = (W - 1) * S
    rows = per_span * hh
    N = spans * per_span
    n0 = max(hh - 2 * A, 0)
    g, c, w, s = (lax.axis_index(a) for a in ("groups", "ctx", "wt", "sub"))
    me = w * S + s
    odd = lax.rem(c, 2)
    base = g * A if Y else 0
    other = (G - 1 - g) * A if Y else 0

    def head(p):
        return p + odd * (hh - 1 - 2 * p) if Z else p

    def rowsof(k):
        return pl.ds(pl.multiple_of(k * R, R), R)

    def shift(i, d, n):
        return lax.rem(i + d + n, n)

    def inside(p):
        return jnp.logical_and(p >= 0, p < C)

    def both(a, b):
        return jnp.logical_and(a, b)

    locals_ = [
        pltpu.make_async_copy(sel_hbm, sel_sm, loc_sem.at[0]),
        pltpu.make_async_copy(cache_hbm, cache_v, loc_sem.at[1]),
        pltpu.make_async_copy(q_hbm, q_v, loc_sem.at[2]),
        pltpu.make_async_copy(
            up_hbm.at[pl.ds(pl.multiple_of(me * hh, hh), hh)], up_v.at[:, rowsof(me)], loc_sem.at[3]
        ),
    ]
    for copy in locals_:
        copy.start()

    barrier = pltpu.get_barrier_semaphore()
    for dw in range(W):
        for ds in range(S):
            if dw or ds:
                pl.semaphore_signal(
                    barrier, inc=1, device_id={"wt": shift(w, dw, W), "sub": shift(s, ds, S)},
                    device_id_type=MESH,
                )
    for dg in range(1, G):
        pl.semaphore_signal(barrier, inc=1, device_id={"groups": shift(g, dg, G)}, device_id_type=MESH)
    for step in (-1, 1):
        @pl.when(inside(c + step))
        def _():
            pl.semaphore_signal(barrier, inc=1, device_id={"ctx": c + step}, device_id_type=MESH)
    beside = (c > 0).astype(jnp.int32) + (c < C - 1).astype(jnp.int32)
    pl.semaphore_wait(barrier, W * S - 1 + G - 1 + beside)

    def x_copy(r, j, sending):
        dw, ds = r // S + 1, r % S
        if sending:
            w2, s2 = shift(w, dw, W), shift(s, ds, S)
            src_k, dst_k = me, w2 * S + s2
        else:
            w2, s2 = shift(w, -dw, W), shift(s, -ds, S)
            src_k, dst_k = w2 * S + s2, me
        h = head(base + j)
        return pltpu.make_async_remote_copy(
            up_hbm.at[dst_k * hh + h], up_v.at[h, rowsof(src_k)],
            x_snd.at[r, j], x_rcv.at[r, j],
            device_id={"wt": w2, "sub": s2}, device_id_type=MESH,
        )

    def far_rows(r):
        dw, ds = r // S + 1, r % S
        return rowsof(shift(w, -dw, W) * S + shift(s, -ds, S))

    def s_copy(ds, sending):
        s2 = shift(s, ds if sending else -ds, S)
        src_s, dst_s = (s, s2) if sending else (s2, s)
        start = pl.multiple_of((w * S + dst_s) * hh, hh)
        return pltpu.make_async_remote_copy(
            up_hbm.at[pl.ds(start, hh)], up_v.at[:, rowsof(w * S + src_s)],
            s_snd.at[ds - 1], s_rcv.at[ds - 1], device_id={"sub": s2}, device_id_type=MESH,
        )

    def y_copy(r, j, sending):
        region = up_v.at[head((base if sending else other) + j), far_rows(r)]
        return pltpu.make_async_remote_copy(
            region, region, y_snd.at[r, j], y_rcv.at[r, j],
            device_id={"groups": G - 1 - g}, device_id_type=MESH,
        )

    def z_from(j):
        return j if j < n0 else j + g * A

    def z_copy(r, j, sending):
        p = z_from(j)
        region = up_v.at[head(p if sending else hh - 1 - p), far_rows(r)]
        return pltpu.make_async_remote_copy(
            region, region, z_snd.at[r, j], z_rcv.at[r, j],
            device_id={"ctx": c + 1 - 2 * odd}, device_id_type=MESH,
        )

    def step_of(way):
        return 2 * way - 1

    def sel_copy(way, d):
        src = sel_hbm if d == 1 else sel_in.at[way, d - 2]
        return pltpu.make_async_remote_copy(
            src, sel_in.at[way, d - 1], sel_snd.at[way, d - 1], sel_rcv.at[way, d - 1],
            device_id={"ctx": c + step_of(way)}, device_id_type=MESH,
        )

    def sel_sends(way, d):
        return both(inside(c + step_of(way)), inside(c - (d - 1) * step_of(way)))

    def k_copy(way, d, i, sending):
        p = c + d * step_of(way) * (1 if sending else -1)
        first = (c if sending else p) * slots + s * half
        return pltpu.make_async_remote_copy(
            send_v.at[way, d - 1, i], kbufs[i].at[pl.ds(first, half)],
            k_snd.at[way, d - 1, i], k_rcv.at[way, d - 1, i], device_id={"ctx": p}, device_id_type=MESH,
        )

    def f_copy(way, d, i, ds, sending):
        owner = c - d * step_of(way)
        s2 = shift(s, ds if sending else -ds, S)
        region = kbufs[i].at[pl.ds(owner * slots + (s if sending else s2) * half, half)]
        return pltpu.make_async_remote_copy(
            region, region, f_snd.at[way, d - 1, i, ds - 1], f_rcv.at[way, d - 1, i, ds - 1],
            device_id={"sub": s2}, device_id_type=MESH,
        )

    for way in range(2):
        pl.when(sel_sends(way, 1))(sel_copy(way, 1).start)
    for j in range(A):
        for r in range(RX):
            x_copy(r, j, True).start()
    for ds in range(1, S):
        s_copy(ds, True).start()

    last = cache_v.shape[0] - 1

    def block(entry):
        return cache_v[jnp.clip(entry, 0, last)]

    locals_[0].wait()
    locals_[1].wait()
    for i in range(spans):
        for t in range(slots):
            kbufs[i][c * slots + t] = block(sel_sm[i, t, c])

    def round_(d):
        for way in range(2):
            @pl.when(inside(c - d * step_of(way)))
            def _():
                sel_copy(way, d).wait_recv()
                if d < C - 1:
                    pl.when(inside(c + step_of(way)))(sel_copy(way, d + 1).start)
                here = pltpu.make_async_copy(
                    sel_in.at[way, d - 1], sel_far.at[way, d - 1], sel_loc.at[way, d - 1]
                )
                here.start()
                here.wait()
                for i in range(spans):
                    for t in range(half):
                        send_v[1 - way, d - 1, i, t] = block(sel_far[way, d - 1, i, s * half + t, c])
                    k_copy(1 - way, d, i, True).start()

    def x_recv(j):
        for r in range(RX):
            x_copy(r, j, False).wait_recv()
            if j < Y:
                y_copy(r, j, True).start()
            if n0 <= j < Z:
                z_copy(r, j, True).start()
            elif j < Z:
                pl.when(g == 0)(z_copy(r, j, True).start)

    def y_recv(j):
        for r in range(RX):
            y_copy(r, j, False).wait_recv()
            if j < min(n0, Z):
                pl.when(g > 0)(z_copy(r, j, True).start)

    def z_recv(j):
        for r in range(RX):
            z_copy(r, j, False).wait_recv()

    def k_recv(d):
        for i in range(spans):
            for way in range(2):
                @pl.when(inside(c - d * step_of(way)))
                def _():
                    k_copy(way, d, i, False).wait_recv()
                    for ds in range(1, S):
                        f_copy(way, d, i, ds, True).start()

    scale = jnp.float32((NOPE + ROPE) ** (-0.5))
    tile = 8 * hh

    def collect(i):
        for d in range(1, C):
            for way in range(2):
                for ds in range(1, S):
                    pl.when(inside(c - d * step_of(way)))(f_copy(way, d, i, ds, False).wait_recv)
        total = C * slots

        def find(n, carry):
            rank, picks = carry
            live = sel_sm[i, lax.rem(n, slots), n // slots] >= 0
            picks = tuple(
                jnp.where(both(live, rank == at), n, old) for at, old in enumerate(picks)
            )
            return rank + live.astype(jnp.int32), picks

        zero = jnp.int32(0)
        _, picks = lax.fori_loop(0, total, find, (zero, (zero,) * C))
        for at in range(C):
            keys_v[at * blk : (at + 1) * blk, :] = kbufs[i][picks[at]]

    def attend(i, first, last):
        @pl.loop(first, last)
        def _(at):
            top = pl.multiple_of(i * rows + at * tile, tile)
            keys = keys_v[...]
            scores = lax.dot_general(
                q_v[pl.ds(top, tile), :], keys, (((1,), (1,)), ((), ())),
                preferred_element_type=jnp.float32,
            ) * scale
            expo = jnp.exp(scores - jnp.max(scores, axis=1, keepdims=True))
            totals = jnp.sum(expo, axis=1, keepdims=True)
            latent = jnp.dot(
                expo.astype(jnp.bfloat16), keys[:, :LAT], preferred_element_type=jnp.float32
            ) / totals
            for l in range(LAT // 128):
                for n in range(8):
                    at_row = pl.multiple_of((i * per_span + at * 8 + n) * stride, 8)
                    lat_v[l, pl.ds(at_row, hh), :] = latent[n * hh : (n + 1) * hh, l * 128 : (l + 1) * 128]

    def project(heads):
        for h in heads:
            left = jnp.concatenate(
                [lat_v[l, pl.ds(h, N, stride=stride), :].astype(jnp.bfloat16) for l in range(LAT // 128)],
                axis=1,
            )
            res_v[pl.ds(h, N, stride=stride), :] = jnp.dot(
                left, up_v[h], preferred_element_type=jnp.float32
            )

    def x_heads(first, last):
        return [head(base + j) for j in range(first, last)]

    def y_heads(first, last):
        return [head(other + j) for j in range(first, last)]

    def z_heads(first, last):
        return [head(hh - 1 - z_from(j)) for j in range(first, last)]

    at_x = at_y = 0
    for d in range(1, C):
        round_(d)
        if at_x < A:
            x_recv(at_x)
            at_x += 1
    for d in range(1, C):
        k_recv(d)
        for _ in range(2):
            if at_x < A // 2:
                x_recv(at_x)
                at_x += 1
        if at_y < min(n0, Y):
            y_recv(at_y)
            at_y += 1
    while at_y < min(n0, Y):
        y_recv(at_y)
        at_y += 1
    locals_[2].wait()
    steps = per_span // 8
    pieces = [(i, k) for i in range(spans) for k in range(steps)]
    served = at_x
    for at, (i, k) in enumerate(pieces):
        if k == 0:
            collect(i)
        attend(i, k, k + 1)
        due = served + (A - 2 - served) * (at + 1) // len(pieces)
        while at_x < due:
            x_recv(at_x)
            at_x += 1

    locals_[3].wait()
    for ds in range(1, S):
        s_copy(ds, False).wait_recv()

    y_done = max(Y - 3, at_y)
    for j in range(at_y, y_done):
        y_recv(j)
    z_done = max(Z - 2, 0)
    for j in range(z_done):
        z_recv(j)
    project(x_heads(0, at_x))
    while at_x < A:
        x_recv(at_x)
        at_x += 1
    project(y_heads(0, y_done) + z_heads(0, z_done))
    for j in range(z_done, Z):
        z_recv(j)
    for j in range(y_done, Y):
        y_recv(j)
    project(x_heads(A - 2, A) + z_heads(z_done, Z) + y_heads(y_done, Y))

    for way in range(2):
        for d in range(1, C):
            pl.when(sel_sends(way, d))(sel_copy(way, d).wait_send)
            for i in range(spans):
                pl.when(inside(c + d * step_of(way)))(k_copy(way, d, i, True).wait_send)
                for ds in range(1, S):
                    pl.when(inside(c - d * step_of(way)))(f_copy(way, d, i, ds, True).wait_send)
    for ds in range(1, S):
        s_copy(ds, True).wait_send()
    for r in range(RX):
        for j in range(A):
            x_copy(r, j, True).wait_send()
        for j in range(Y):
            y_copy(r, j, True).wait_send()
        for j in range(Z):
            z_copy(r, j, True).wait_send()


def finish(stride, res_ref, out_ref):
    hh = out_ref.shape[1]

    @pl.loop(0, out_ref.shape[0])
    def _(n):
        out_ref[n] = res_ref[pl.ds(pl.multiple_of(n * stride, 8), hh), :].astype(jnp.bfloat16)


def split(G, C, hh):
    if G != 2 or C % 2 or hh < 8:
        return hh, 0, 0
    A = (14 * hh) // 32
    Y = (12 * hh) // 32
    return A, Y, hh - A - Y


def per_device(queries, selection, latent_cache, value_up):
    G, C, W, S = (lax.axis_size(a) for a in ("groups", "ctx", "wt", "sub"))
    spans, per_span, hh, width = queries.shape
    slots = selection.shape[2]
    blk = latent_cache.shape[1]
    R, V = value_up.shape[1:]
    A, Y, Z = split(G, C, hh)
    stride = hh + 8
    N = spans * per_span
    RX = (W - 1) * S
    half = slots // S
    far = max(C - 1, 1)
    dims = (G, C, W, S, spans, per_span, hh, slots, blk, width, R, V, stride, A, Y, Z)
    bf16, dma = jnp.bfloat16, pltpu.SemaphoreType.DMA
    hbm = pl.BlockSpec(memory_space=pltpu.HBM)
    vmem = pl.BlockSpec(memory_space=pltpu.VMEM)
    given = (selection.transpose(0, 2, 1), queries.reshape(N * hh, width), latent_cache, value_up)
    res = pl.pallas_call(
        functools.partial(kernel, dims),
        out_shape=pltpu.VMEM((N * stride, V), jnp.float32),
        in_specs=[hbm] * 4,
        out_specs=vmem,
        scratch_shapes=[
            pltpu.VMEM((N * hh, width), bf16),
            pltpu.VMEM(latent_cache.shape, bf16),
            pltpu.VMEM((hh, LAT, V), bf16),
            pltpu.SMEM((spans, slots, C), jnp.int32),
            pltpu.VMEM((2, far, spans, slots, C), jnp.int32),
            pltpu.SMEM((2, far, spans, slots, C), jnp.int32),
            pltpu.VMEM((2, far, spans, half, blk, width), bf16),
            pltpu.VMEM((C * blk, width), bf16),
            pltpu.VMEM((LAT // 128, N * stride, 128), jnp.float32),
            *[pltpu.VMEM((C * slots, blk, width), bf16) for _ in range(spans)],
            dma((4,)), dma((2, far)), dma((2, far)), dma((2, far)),
            dma((RX, A)), dma((RX, A)), dma((max(S - 1, 1),)), dma((max(S - 1, 1),)),
            dma((RX, max(Y, 1))), dma((RX, max(Y, 1))),
            dma((2, far, spans)), dma((2, far, spans)),
            dma((2, far, spans, max(S - 1, 1))), dma((2, far, spans, max(S - 1, 1))),
            dma((RX, max(Z, 1))), dma((RX, max(Z, 1))),
        ],
        compiler_params=pltpu.CompilerParams(
            collective_id=0, has_side_effects=True, vmem_limit_bytes=48 * 1024 * 1024
        ),
    )(*(pltpu.with_memory_space_constraint(a, pltpu.HBM) for a in given))
    out = pl.pallas_call(
        functools.partial(finish, stride),
        out_shape=jax.ShapeDtypeStruct((N, hh, V), bf16),
        in_specs=[vmem],
        out_specs=vmem,
        compiler_params=pltpu.CompilerParams(vmem_limit_bytes=8 * 1024 * 1024),
    )(res)
    return out.reshape(spans, per_span, hh, V)


def solution(mesh):
    placed = (
        P(("groups", "ctx"), None, ("wt", "sub"), None),
        P(("groups", "ctx"), None, None),
        P(("groups", "ctx"), None, None),
        P(None, ("wt", "sub"), None),
    )
    return jax.shard_map(
        per_device,
        mesh=mesh,
        in_specs=placed,
        out_specs=P(("groups", "ctx"), None, ("wt", "sub"), None),
        check_vma=False,
    )
```

```python
import functools

import jax
import jax.numpy as jnp
from jax import lax
from jax.experimental import pallas as pl
from jax.experimental.pallas import tpu as pltpu
from jax.sharding import PartitionSpec as P

LAT = 512
ROPE = 64
NOPE = 128
MESH = pl.DeviceIdType.MESH
T_K0, T_K1, T_F = 15.0, 6.7, 0.3


def kernel(
    dims, sel_hbm, q_hbm, cache_hbm, up_hbm, res_v,
    q_v, cache_v, up_v, sel_sm, sel_far, send_v, keys_v, lat_v, *rest,
):
    (G, C, W, S, spans, per_span, hh, slots, blk, width, R, V, stride, A, Y, Z) = dims
    kbufs = rest[:spans]
    (known, loc_sem, sel_snd, sel_rcv, x_snd, x_rcv, s_snd, s_rcv, y_snd, y_rcv,
     k_snd, k_rcv, f_snd, f_rcv, z_snd, z_rcv) = rest[spans:]
    half = slots // S
    groups = LAT // ROPE
    RX = (W - 1) * S
    rows = per_span * hh
    N = spans * per_span
    n0 = max(hh - 2 * A, 0)
    g, c, w, s = (lax.axis_index(a) for a in ("groups", "ctx", "wt", "sub"))
    me = w * S + s
    odd = lax.rem(c, 2)
    base = g * A if Y else 0
    other = (G - 1 - g) * A if Y else 0

    def head(p):
        return p + odd * (hh - 1 - 2 * p) if Z else p

    def rowsof(k):
        return pl.ds(pl.multiple_of(k * R, R), R)

    def shift(i, d, n):
        return lax.rem(i + d + n, n)

    def inside(p):
        return jnp.logical_and(p >= 0, p < C)

    def both(a, b):
        return jnp.logical_and(a, b)

    locals_ = [
        pltpu.make_async_copy(sel_hbm, sel_sm, loc_sem.at[0]),
        pltpu.make_async_copy(cache_hbm, cache_v, loc_sem.at[1]),
        pltpu.make_async_copy(q_hbm, q_v, loc_sem.at[2]),
        pltpu.make_async_copy(
            up_hbm.at[pl.ds(pl.multiple_of(me * hh, hh), hh)], up_v.at[:, rowsof(me)], loc_sem.at[3]
        ),
    ]
    for copy in locals_:
        copy.start()

    barrier = pltpu.get_barrier_semaphore()
    for dw in range(W):
        for ds in range(S):
            if dw or ds:
                pl.semaphore_signal(
                    barrier, inc=1, device_id={"wt": shift(w, dw, W), "sub": shift(s, ds, S)},
                    device_id_type=MESH,
                )
    for dg in range(1, G):
        pl.semaphore_signal(barrier, inc=1, device_id={"groups": shift(g, dg, G)}, device_id_type=MESH)
    for step in (-1, 1):
        @pl.when(inside(c + step))
        def _():
            pl.semaphore_signal(barrier, inc=1, device_id={"ctx": c + step}, device_id_type=MESH)
    beside = (c > 0).astype(jnp.int32) + (c < C - 1).astype(jnp.int32)
    pl.semaphore_wait(barrier, W * S - 1 + G - 1 + beside)

    def x_copy(r, j, sending):
        dw, ds = r // S + 1, r % S
        if sending:
            w2, s2 = shift(w, dw, W), shift(s, ds, S)
            src_k, dst_k = me, w2 * S + s2
        else:
            w2, s2 = shift(w, -dw, W), shift(s, -ds, S)
            src_k, dst_k = w2 * S + s2, me
        h = head(base + j)
        return pltpu.make_async_remote_copy(
            up_hbm.at[dst_k * hh + h], up_v.at[h, rowsof(src_k)],
            x_snd.at[r, j], x_rcv.at[r, j],
            device_id={"wt": w2, "sub": s2}, device_id_type=MESH,
        )

    def far_rows(r):
        dw, ds = r // S + 1, r % S
        return rowsof(shift(w, -dw, W) * S + shift(s, -ds, S))

    def s_copy(ds, sending):
        s2 = shift(s, ds if sending else -ds, S)
        src_s, dst_s = (s, s2) if sending else (s2, s)
        start = pl.multiple_of((w * S + dst_s) * hh, hh)
        return pltpu.make_async_remote_copy(
            up_hbm.at[pl.ds(start, hh)], up_v.at[:, rowsof(w * S + src_s)],
            s_snd.at[ds - 1], s_rcv.at[ds - 1], device_id={"sub": s2}, device_id_type=MESH,
        )

    def y_copy(r, j, sending):
        region = up_v.at[head((base if sending else other) + j), far_rows(r)]
        return pltpu.make_async_remote_copy(
            region, region, y_snd.at[r, j], y_rcv.at[r, j],
            device_id={"groups": G - 1 - g}, device_id_type=MESH,
        )

    def z_from(j):
        return j if j < n0 else j + g * A

    def z_copy(r, j, sending):
        p = z_from(j)
        region = up_v.at[head(p if sending else hh - 1 - p), far_rows(r)]
        return pltpu.make_async_remote_copy(
            region, region, z_snd.at[r, j], z_rcv.at[r, j],
            device_id={"ctx": c + 1 - 2 * odd}, device_id_type=MESH,
        )

    def step_of(way):
        return 2 * way - 1

    def sel_copy(way, d):
        return pltpu.make_async_remote_copy(
            sel_hbm, sel_far.at[way, d - 1], sel_snd.at[way, d - 1], sel_rcv.at[way, d - 1],
            device_id={"ctx": c + d * step_of(way)}, device_id_type=MESH,
        )

    def announce(d):
        for way in range(2):
            @pl.when(inside(c - d * step_of(way)))
            def _():
                if d > 1:
                    pl.semaphore_wait(known.at[way, d - 1], 1)
                if d < C - 1:
                    @pl.when(inside(c + step_of(way)))
                    def _():
                        pl.semaphore_signal(
                            known.at[way, d], inc=1, device_id={"ctx": c + step_of(way)}, device_id_type=MESH
                        )
                sel_copy(1 - way, d).start()

    def k_copy(way, d, i, sending):
        p = c + d * step_of(way) * (1 if sending else -1)
        first = (c if sending else p) * slots + s * half
        return pltpu.make_async_remote_copy(
            send_v.at[way, d - 1, i], kbufs[i].at[pl.ds(first, half)],
            k_snd.at[way, d - 1, i], k_rcv.at[way, d - 1, i], device_id={"ctx": p}, device_id_type=MESH,
        )

    def f_copy(way, d, i, ds, sending):
        owner = c - d * step_of(way)
        s2 = shift(s, ds if sending else -ds, S)
        region = kbufs[i].at[pl.ds(owner * slots + (s if sending else s2) * half, half)]
        return pltpu.make_async_remote_copy(
            region, region, f_snd.at[way, d - 1, i, ds - 1], f_rcv.at[way, d - 1, i, ds - 1],
            device_id={"sub": s2}, device_id_type=MESH,
        )

    if C > 1:
        announce(1)
    for j in range(A):
        for r in range(RX):
            x_copy(r, j, True).start()
    for d in range(2, C):
        announce(d)
    for ds in range(1, S):
        s_copy(ds, True).start()

    last = cache_v.shape[0] - 1

    tall = blk // groups

    def pack(dst, entry):
        n = jnp.clip(entry, 0, last)
        dst[:blk, :] = cache_v[n, :, :LAT]
        dst[blk:, :] = jnp.concatenate(
            [cache_v[n, q * tall : (q + 1) * tall, LAT:] for q in range(groups)], axis=1
        )

    def round_(d):
        for way in range(2):
            @pl.when(inside(c - d * step_of(way)))
            def _():
                sel_copy(way, d).wait_recv()
                for i in range(spans):
                    for t in range(half):
                        pack(send_v.at[1 - way, d - 1, i, t], sel_far[way, d - 1, i, s * half + t, c])
                    k_copy(1 - way, d, i, True).start()

    def x_recv(j):
        for r in range(RX):
            x_copy(r, j, False).wait_recv()
            if j < Y:
                y_copy(r, j, True).start()

    def x_pass(j):
        for r in range(RX):
            if j >= n0:
                z_copy(r, j, True).start()
            else:
                pl.when(g == 0)(z_copy(r, j, True).start)

    def y_recv(j):
        for r in range(RX):
            y_copy(r, j, False).wait_recv()

    def y_pass(j):
        @pl.when(g > 0)
        def _():
            y_recv(j)
            for r in range(RX):
                z_copy(r, j, True).start()

    def y_late(j):
        pl.when(g == 0)(lambda: y_recv(j))

    def z_recv(j):
        for r in range(RX):
            z_copy(r, j, False).wait_recv()

    def k_recv(d):
        for i in range(spans):
            for way in range(2):
                @pl.when(inside(c - d * step_of(way)))
                def _():
                    k_copy(way, d, i, False).wait_recv()
                    for ds in range(1, S):
                        f_copy(way, d, i, ds, True).start()

    scale = jnp.float32((NOPE + ROPE) ** (-0.5))
    share = min(16, per_span)
    tile = share * hh

    def collect(i):
        for d in range(1, C):
            for way in range(2):
                for ds in range(1, S):
                    pl.when(inside(c - d * step_of(way)))(f_copy(way, d, i, ds, False).wait_recv)
        total = C * slots

        def find(n, carry):
            rank, picks = carry
            live = sel_sm[i, lax.rem(n, slots), n // slots] >= 0
            picks = tuple(
                jnp.where(both(live, rank == at), n, old) for at, old in enumerate(picks)
            )
            return rank + live.astype(jnp.int32), picks

        zero = jnp.int32(0)
        _, picks = lax.fori_loop(0, total, find, (zero, (zero,) * C))
        for at in range(C):
            keys_v[at * blk : (at + 1) * blk, :LAT] = kbufs[i][picks[at], :blk, :]
            for q in range(groups):
                low = at * blk + q * tall
                keys_v[low : low + tall, LAT:] = kbufs[i][picks[at], blk:, q * ROPE : (q + 1) * ROPE]

    def attend(i):
        for at in range(per_span // share):
            top = i * rows + at * tile
            keys = keys_v[...]
            scores = lax.dot_general(
                q_v[top : top + tile, :], keys, (((1,), (1,)), ((), ())),
                preferred_element_type=jnp.float32,
            ) * scale
            expo = jnp.exp(scores - jnp.max(scores, axis=1, keepdims=True))
            totals = jnp.sum(expo, axis=1, keepdims=True)
            latent = jnp.dot(
                expo.astype(jnp.bfloat16), keys[:, :LAT], preferred_element_type=jnp.float32
            ) / totals
            for l in range(LAT // 128):
                for n in range(share):
                    at_row = (i * per_span + at * share + n) * stride
                    lat_v[l, at_row : at_row + hh, :] = latent[n * hh : (n + 1) * hh, l * 128 : (l + 1) * 128]

    def project(heads):
        for h in heads:
            left = jnp.concatenate(
                [lat_v[l, pl.ds(h, N, stride=stride), :].astype(jnp.bfloat16) for l in range(LAT // 128)],
                axis=1,
            )
            res_v[pl.ds(h, N, stride=stride), :] = jnp.dot(
                left, up_v[h], preferred_element_type=jnp.float32
            )

    def prepare():
        locals_[0].wait()
        for i in range(spans):
            for t in range(slots):
                pack(kbufs[i].at[c * slots + t], sel_sm[i, t, c])
        locals_[2].wait()

    def ready():
        locals_[3].wait()
        for ds in range(1, S):
            s_copy(ds, False).wait_recv()

    events = []

    def at(time, act, *args):
        events.append((time, len(events), act, args))

    unit, lead = 1.43 * 32 / hh, 7.0
    keys_at = [T_K0 + T_K1 * (d + 1) / (C - 1) for d in range(C - 1)]
    start = keys_at[-1] + T_F if C > 1 else lead
    done = start + 1.3 * spans
    locals_[1].wait()
    for d in range(1, C):
        at(lead + (1.0 * d - 2.0 if C < 8 else 0.0), round_, d)
        at(keys_at[d - 1], k_recv, d)
    at(lead + 0.5, prepare)
    for i in range(spans):
        at(start + 1.3 * i, collect, i)
        at(start + 1.3 * i, attend, i)
    at(done, ready)
    for j in range(A):
        x_at = lead + unit * j
        at(x_at, x_recv, j)
        if j < Z:
            at(max(x_at, lead + 2.0), x_pass, j)
        at(max(x_at, done), project, head(base + j))
        if j < Y:
            y_at = x_at + 3.5
            if j < min(n0, Z):
                at(y_at + 1.0, y_pass, j)
                at(max(y_at, done), y_late, j)
            else:
                at(max(y_at, done), y_recv, j)
            at(max(y_at, done), project, head(other + j))
    for j in range(Z):
        z_at = max(lead + unit * (A - 1 - (Z - 1 - j)), done)
        at(z_at, z_recv, j)
        at(z_at, project, head(hh - 1 - z_from(j)))
    events.sort(key=lambda e: e[:2])
    heads = []
    for _, _, act, args in events:
        if act is project:
            heads.extend(args)
            if len(heads) < 8:
                continue
        if act is project:
            project(heads)
            heads = []
        else:
            act(*args)
    project(heads)

    for way in range(2):
        for d in range(1, C):
            pl.when(inside(c + d * step_of(way)))(sel_copy(way, d).wait_send)
            for i in range(spans):
                pl.when(inside(c + d * step_of(way)))(k_copy(way, d, i, True).wait_send)
                for ds in range(1, S):
                    pl.when(inside(c - d * step_of(way)))(f_copy(way, d, i, ds, True).wait_send)
    for ds in range(1, S):
        s_copy(ds, True).wait_send()
    for r in range(RX):
        for j in range(A):
            x_copy(r, j, True).wait_send()
        for j in range(Y):
            y_copy(r, j, True).wait_send()
        for j in range(Z):
            z_copy(r, j, True).wait_send()


def finish(stride, res_ref, out_ref):
    hh = out_ref.shape[1]

    @pl.loop(0, out_ref.shape[0])
    def _(n):
        out_ref[n] = res_ref[pl.ds(pl.multiple_of(n * stride, 8), hh), :].astype(jnp.bfloat16)


def split(G, C, hh):
    if G != 2 or C % 2 or hh < 8:
        return hh, 0, 0
    A = (15 * hh) // 32
    Y = (11 * hh) // 32
    return A, Y, hh - A - Y


def per_device(queries, selection, latent_cache, value_up):
    G, C, W, S = (lax.axis_size(a) for a in ("groups", "ctx", "wt", "sub"))
    spans, per_span, hh, width = queries.shape
    slots = selection.shape[2]
    blk = latent_cache.shape[1]
    R, V = value_up.shape[1:]
    A, Y, Z = split(G, C, hh)
    stride = hh + 8
    N = spans * per_span
    RX = (W - 1) * S
    half = slots // S
    high = blk + blk * ROPE // LAT
    far = max(C - 1, 1)
    dims = (G, C, W, S, spans, per_span, hh, slots, blk, width, R, V, stride, A, Y, Z)
    bf16, dma = jnp.bfloat16, pltpu.SemaphoreType.DMA
    hbm = pl.BlockSpec(memory_space=pltpu.HBM)
    vmem = pl.BlockSpec(memory_space=pltpu.VMEM)
    given = (selection.transpose(0, 2, 1), queries.reshape(N * hh, width), latent_cache, value_up)
    res = pl.pallas_call(
        functools.partial(kernel, dims),
        out_shape=pltpu.VMEM((N * stride, V), jnp.float32),
        in_specs=[hbm] * 4,
        out_specs=vmem,
        scratch_shapes=[
            pltpu.VMEM((N * hh, width), bf16),
            pltpu.VMEM(latent_cache.shape, bf16),
            pltpu.VMEM((hh, LAT, V), bf16),
            pltpu.SMEM((spans, slots, C), jnp.int32),
            pltpu.SMEM((2, far, spans, slots, C), jnp.int32),
            pltpu.VMEM((2, far, spans, half, high, LAT), bf16),
            pltpu.VMEM((C * blk, width), bf16),
            pltpu.VMEM((LAT // 128, N * stride, 128), jnp.float32),
            *[pltpu.VMEM((C * slots, high, LAT), bf16) for _ in range(spans)],
            pltpu.SemaphoreType.REGULAR((2, far)), dma((4,)), dma((2, far)), dma((2, far)),
            dma((RX, A)), dma((RX, A)), dma((max(S - 1, 1),)), dma((max(S - 1, 1),)),
            dma((RX, max(Y, 1))), dma((RX, max(Y, 1))),
            dma((2, far, spans)), dma((2, far, spans)),
            dma((2, far, spans, max(S - 1, 1))), dma((2, far, spans, max(S - 1, 1))),
            dma((RX, max(Z, 1))), dma((RX, max(Z, 1))),
        ],
        compiler_params=pltpu.CompilerParams(
            collective_id=0, has_side_effects=True, vmem_limit_bytes=48 * 1024 * 1024
        ),
    )(*(pltpu.with_memory_space_constraint(a, pltpu.HBM) for a in given))
    out = pl.pallas_call(
        functools.partial(finish, stride),
        out_shape=jax.ShapeDtypeStruct((N, hh, V), bf16),
        in_specs=[vmem],
        out_specs=vmem,
        compiler_params=pltpu.CompilerParams(vmem_limit_bytes=8 * 1024 * 1024),
    )(res)
    return out.reshape(spans, per_span, hh, V)


def solution(mesh):
    placed = (
        P(("groups", "ctx"), None, ("wt", "sub"), None),
        P(("groups", "ctx"), None, None),
        P(("groups", "ctx"), None, None),
        P(None, ("wt", "sub"), None),
    )
    return jax.shard_map(
        per_device,
        mesh=mesh,
        in_specs=placed,
        out_specs=P(("groups", "ctx"), None, ("wt", "sub"), None),
        check_vma=False,
    )
```

```python
import functools
import itertools

import jax
import jax.numpy as jnp
from jax import lax
from jax.experimental import pallas as pl
from jax.experimental.pallas import tpu as pltpu
from jax.sharding import PartitionSpec as P

LAT = 512
ROPE = 64
NOPE = 128
MESH = pl.DeviceIdType.MESH
T_K0, T_K1, T_F, T_P = 15.0, 6.5, 0.3, 14


def kernel(
    dims, sel_hbm, q_hbm, cache_hbm, up_hbm, res_v,
    q_v, cache_v, up_v, sel_sm, chosen, sel_far, send_v, keys_v, lat_v, kbuf,
    known, loc_sem, sel_snd, sel_rcv, x_snd, x_rcv, s_snd, s_rcv, y_snd, y_rcv,
    k_snd, k_rcv, f_snd, f_rcv, z_snd, z_rcv,
):
    (G, C, W, S, spans, per_span, hh, slots, blk, width, R, V, stride, A, Y, Z) = dims
    half = slots // S
    groups = LAT // ROPE
    RX = (W - 1) * S
    rows = per_span * hh
    N = spans * per_span
    n0 = max(hh - 2 * A, 0)
    g, c, w, s = (lax.axis_index(a) for a in ("groups", "ctx", "wt", "sub"))
    me = w * S + s
    odd = lax.rem(c, 2)
    base = g * A if Y else 0
    other = (G - 1 - g) * A if Y else 0

    def head(p):
        return p + odd * (hh - 1 - 2 * p) if Z else p

    def rowsof(k):
        return pl.ds(pl.multiple_of(k * R, R), R)

    def shift(i, d, n):
        return lax.rem(i + d + n, n)

    def inside(p):
        return jnp.logical_and(p >= 0, p < C)

    def both(a, b):
        return jnp.logical_and(a, b)

    locals_ = [
        pltpu.make_async_copy(sel_hbm, sel_sm, loc_sem.at[0]),
        pltpu.make_async_copy(cache_hbm, cache_v, loc_sem.at[1]),
        pltpu.make_async_copy(q_hbm, q_v, loc_sem.at[2]),
        pltpu.make_async_copy(
            up_hbm.at[pl.ds(pl.multiple_of(me * hh, hh), hh)], up_v.at[:, rowsof(me)], loc_sem.at[3]
        ),
    ]
    for copy in locals_:
        copy.start()

    barrier = pltpu.get_barrier_semaphore()
    for dw in range(W):
        for ds in range(S):
            if dw or ds:
                pl.semaphore_signal(
                    barrier, inc=1, device_id={"wt": shift(w, dw, W), "sub": shift(s, ds, S)},
                    device_id_type=MESH,
                )
    for dg in range(1, G):
        pl.semaphore_signal(barrier, inc=1, device_id={"groups": shift(g, dg, G)}, device_id_type=MESH)
    for step in (-1, 1):
        @pl.when(inside(c + step))
        def _():
            pl.semaphore_signal(barrier, inc=1, device_id={"ctx": c + step}, device_id_type=MESH)
    beside = (c > 0).astype(jnp.int32) + (c < C - 1).astype(jnp.int32)
    pl.semaphore_wait(barrier, W * S - 1 + G - 1 + beside)

    def x_copy(r, j, sending):
        dw, ds = r // S + 1, r % S
        if sending:
            w2, s2 = shift(w, dw, W), shift(s, ds, S)
            src_k, dst_k = me, w2 * S + s2
        else:
            w2, s2 = shift(w, -dw, W), shift(s, -ds, S)
            src_k, dst_k = w2 * S + s2, me
        h = head(base + j)
        return pltpu.make_async_remote_copy(
            up_hbm.at[dst_k * hh + h], up_v.at[h, rowsof(src_k)],
            x_snd.at[0], x_rcv.at[j],
            device_id={"wt": w2, "sub": s2}, device_id_type=MESH,
        )

    def far_rows(r):
        dw, ds = r // S + 1, r % S
        return rowsof(shift(w, -dw, W) * S + shift(s, -ds, S))

    def s_copy(ds, sending):
        s2 = shift(s, ds if sending else -ds, S)
        src_s, dst_s = (s, s2) if sending else (s2, s)
        start = pl.multiple_of((w * S + dst_s) * hh, hh)
        return pltpu.make_async_remote_copy(
            up_hbm.at[pl.ds(start, hh)], up_v.at[:, rowsof(w * S + src_s)],
            s_snd.at[ds - 1], s_rcv.at[ds - 1], device_id={"sub": s2}, device_id_type=MESH,
        )

    def y_copy(r, j, sending):
        region = up_v.at[head((base if sending else other) + j), far_rows(r)]
        return pltpu.make_async_remote_copy(
            region, region, y_snd.at[0], y_rcv.at[j],
            device_id={"groups": G - 1 - g}, device_id_type=MESH,
        )

    def z_from(j):
        return j if j < n0 else j + g * A

    def z_copy(r, j, sending):
        p = z_from(j)
        region = up_v.at[head(p if sending else hh - 1 - p), far_rows(r)]
        return pltpu.make_async_remote_copy(
            region, region, z_snd.at[0], z_rcv.at[j],
            device_id={"ctx": c + 1 - 2 * odd}, device_id_type=MESH,
        )

    def step_of(way):
        return 2 * way - 1

    def sel_copy(way, d):
        return pltpu.make_async_remote_copy(
            sel_hbm, sel_far.at[way, d - 1], sel_snd.at[0], sel_rcv.at[way, d - 1],
            device_id={"ctx": c + d * step_of(way)}, device_id_type=MESH,
        )

    def announce(d):
        for way in range(2):
            @pl.when(inside(c - d * step_of(way)))
            def _():
                if d > 1:
                    pl.semaphore_wait(known.at[way, d - 1], 1)
                if d < C - 1:
                    @pl.when(inside(c + step_of(way)))
                    def _():
                        pl.semaphore_signal(
                            known.at[way, d], inc=1, device_id={"ctx": c + step_of(way)}, device_id_type=MESH
                        )
                sel_copy(1 - way, d).start()

    def k_copy(way, d, sending):
        p = c + d * step_of(way) * (1 if sending else -1)
        first = (c if sending else p) * slots + s * half
        return pltpu.make_async_remote_copy(
            send_v.at[way, d - 1], kbuf.at[:, pl.ds(first, half)],
            k_snd.at[0], k_rcv.at[way, d - 1], device_id={"ctx": p}, device_id_type=MESH,
        )

    def f_copy(way, d, ds, sending):
        owner = c - d * step_of(way)
        s2 = shift(s, ds if sending else -ds, S)
        region = kbuf.at[:, pl.ds(owner * slots + (s if sending else s2) * half, half)]
        return pltpu.make_async_remote_copy(
            region, region, f_snd.at[0], f_rcv.at[way, d - 1, ds - 1],
            device_id={"sub": s2}, device_id_type=MESH,
        )

    def drain(region, sem):
        pltpu.make_async_copy(region, region, sem).wait()

    def unit_bytes(n):
        return up_v.at[pl.ds(0, n), pl.ds(0, RX * R)]

    if C > 1:
        announce(1)
    for j in range(A):
        for r in range(RX):
            x_copy(r, j, True).start()
    for d in range(2, C):
        announce(d)
    for ds in range(1, S):
        s_copy(ds, True).start()

    last = cache_v.shape[0] - 1

    tall = blk // groups

    def pack(dst, entry):
        n = jnp.clip(entry, 0, last)
        dst[:blk, :] = cache_v[n, :, :LAT]
        dst[blk:, :] = jnp.concatenate(
            [cache_v[n, q * tall : (q + 1) * tall, LAT:] for q in range(groups)], axis=1
        )

    def round_(d):
        for way in range(2):
            @pl.when(inside(c - d * step_of(way)))
            def _():
                sel_copy(way, d).wait_recv()
                for i in range(spans):
                    for t in range(half):
                        pack(send_v.at[1 - way, d - 1, i, t], sel_far[way, d - 1, i, s * half + t, c])
                k_copy(1 - way, d, True).start()

    def x_recv(j):
        drain(unit_bytes(1), x_rcv.at[j])
        for r in range(RX if j < Y else 0):
            y_copy(r, j, True).start()

    def x_pass(j):
        for r in range(RX):
            if j >= n0:
                z_copy(r, j, True).start()
            else:
                pl.when(g == 0)(z_copy(r, j, True).start)

    def y_recv(j):
        drain(unit_bytes(1), y_rcv.at[j])

    def y_pass(j):
        @pl.when(g > 0)
        def _():
            y_recv(j)
            for r in range(RX):
                z_copy(r, j, True).start()

    def y_late(j):
        pl.when(g == 0)(lambda: y_recv(j))

    def z_recv(j):
        drain(unit_bytes(1), z_rcv.at[j])

    def k_recv(d):
        for way in range(2):
            @pl.when(inside(c - d * step_of(way)))
            def _():
                k_copy(way, d, False).wait_recv()
                for ds in range(1, S):
                    f_copy(way, d, ds, True).start()

    scale = jnp.float32((NOPE + ROPE) ** (-0.5))
    share = min(16, per_span)
    tile = share * hh

    def live_slots(i):
        total = C * slots

        def find(n, carry):
            rank, picks = carry
            live = sel_sm[i, lax.rem(n, slots), n // slots] >= 0
            picks = tuple(
                jnp.where(both(live, rank == at), n, old) for at, old in enumerate(picks)
            )
            return rank + live.astype(jnp.int32), picks

        zero = jnp.int32(0)
        return lax.fori_loop(0, total, find, (zero, (zero,) * C))[1]

    def gathered():
        for d in range(1, C):
            for way in range(2):
                for ds in range(1, S):
                    pl.when(inside(c - d * step_of(way)))(f_copy(way, d, ds, False).wait_recv)

    def collect(i):
        for at in range(C):
            slot = chosen[i, at]
            keys_v[i, at * blk : (at + 1) * blk, :LAT] = kbuf[i, slot, :blk, :]
            for q in range(groups):
                low = at * blk + q * tall
                keys_v[i, low : low + tall, LAT:] = kbuf[i, slot, blk:, q * ROPE : (q + 1) * ROPE]

    def attend():
        for i, at in itertools.product(range(spans), range(per_span // share)):
            top = i * rows + at * tile
            keys = keys_v[i]
            scores = lax.dot_general(
                q_v[top : top + tile, :], keys, (((1,), (1,)), ((), ())),
                preferred_element_type=jnp.float32,
            ) * scale
            expo = jnp.exp(scores - jnp.max(scores, axis=1, keepdims=True))
            totals = jnp.sum(expo, axis=1, keepdims=True)
            latent = jnp.dot(
                expo.astype(jnp.bfloat16), keys[:, :LAT], preferred_element_type=jnp.float32
            ) / totals
            for l in range(LAT // 128):
                for n in range(share):
                    at_row = (i * per_span + at * share + n) * stride
                    lat_v[l, at_row : at_row + hh, :] = latent[n * hh : (n + 1) * hh, l * 128 : (l + 1) * 128]

    def project(heads):
        for h in heads:
            left = jnp.concatenate(
                [lat_v[l, pl.ds(h, N, stride=stride), :].astype(jnp.bfloat16) for l in range(LAT // 128)],
                axis=1,
            )
            res_v[pl.ds(h, N, stride=stride), :] = jnp.dot(
                left, up_v[h], preferred_element_type=jnp.float32
            )

    def prepare():
        locals_[0].wait()
        for i in range(spans):
            for t in range(slots):
                pack(kbuf.at[i, c * slots + t], sel_sm[i, t, c])
            for at, slot in enumerate(live_slots(i)):
                chosen[i, at] = slot
        locals_[2].wait()

    def ready():
        locals_[3].wait()
        for ds in range(1, S):
            s_copy(ds, False).wait_recv()

    events = []

    def at(time, act, *args):
        events.append((time, len(events), act, args))

    unit, lead = 1.43 * 32 / hh, 7.0
    keys_at = [T_K0 + T_K1 * (d + 1) / (C - 1) for d in range(C - 1)]
    start = keys_at[-1] + T_F if C > 1 else lead
    done = start + 1.3 * spans
    locals_[1].wait()
    for d in range(1, C):
        at(lead + (1.0 * d - 2.0 if C < 8 else 0.0), round_, d)
        at(keys_at[d - 1], k_recv, d)
    at(lead + 0.5, prepare)
    at(start, gathered)
    for i in range(spans):
        at(start, collect, i)
    at(start, attend)
    at(done, ready)
    for j in range(A):
        x_at = lead + unit * j
        at(x_at, x_recv, j)
        if j < Z:
            at(max(x_at, lead + 2.0), x_pass, j)
        at(max(x_at, done), project, head(base + j))
        if j < Y:
            y_at = x_at + 3.5
            if j < min(n0, Z):
                at(y_at + 1.0, y_pass, j)
                at(max(y_at, done), y_late, j)
            else:
                at(max(y_at, done), y_recv, j)
            at(max(y_at, done), project, head(other + j))
    for j in range(Z):
        z_at = max(lead + unit * (A - 1 - (Z - 1 - j)), done)
        at(z_at, z_recv, j)
        at(z_at, project, head(hh - 1 - z_from(j)))
    events.sort(key=lambda e: e[:2])
    heads = []
    for _, _, act, args in events:
        if act is project:
            heads.extend(args)
            if len(heads) < T_P:
                continue
        if act is project:
            project(heads)
            heads = []
        else:
            act(*args)
    project(heads)

    if C > 1:
        drain(sel_far.at[0], sel_snd.at[0])
        drain(send_v.at[0], k_snd.at[0])
        if S > 1:
            drain(send_v.at[pl.ds(0, S - 1)], f_snd.at[0])
    for ds in range(1, S):
        s_copy(ds, True).wait_send()
    if RX:
        for count, sem in ((A, x_snd), (Y, y_snd), (Z, z_snd)):
            if count:
                drain(unit_bytes(count), sem.at[0])


def finish(stride, res_ref, out_ref):
    hh = out_ref.shape[1]

    for n in range(out_ref.shape[0]):
        out_ref[n] = res_ref[n * stride : n * stride + hh, :].astype(jnp.bfloat16)


def split(G, C, hh):
    if G != 2 or C % 2 or hh < 8:
        return hh, 0, 0
    A = (15 * hh) // 32
    Y = (11 * hh) // 32
    return A, Y, hh - A - Y


def per_device(queries, selection, latent_cache, value_up):
    G, C, W, S = (lax.axis_size(a) for a in ("groups", "ctx", "wt", "sub"))
    spans, per_span, hh, width = queries.shape
    slots = selection.shape[2]
    blk = latent_cache.shape[1]
    R, V = value_up.shape[1:]
    A, Y, Z = split(G, C, hh)
    stride = hh + 8
    N = spans * per_span
    RX = (W - 1) * S
    half = slots // S
    high = blk + blk * ROPE // LAT
    far = max(C - 1, 1)
    dims = (G, C, W, S, spans, per_span, hh, slots, blk, width, R, V, stride, A, Y, Z)
    bf16, dma = jnp.bfloat16, pltpu.SemaphoreType.DMA
    hbm = pl.BlockSpec(memory_space=pltpu.HBM)
    vmem = pl.BlockSpec(memory_space=pltpu.VMEM)
    given = (selection.transpose(0, 2, 1), queries.reshape(N * hh, width), latent_cache, value_up)
    res = pl.pallas_call(
        functools.partial(kernel, dims),
        out_shape=pltpu.VMEM((N * stride, V), jnp.float32),
        in_specs=[hbm] * 4,
        out_specs=vmem,
        scratch_shapes=[
            pltpu.VMEM((N * hh, width), bf16),
            pltpu.VMEM(latent_cache.shape, bf16),
            pltpu.VMEM((hh, LAT, V), bf16),
            pltpu.SMEM((spans, slots, C), jnp.int32),
            pltpu.SMEM((spans, C), jnp.int32),
            pltpu.SMEM((2, far, spans, slots, C), jnp.int32),
            pltpu.VMEM((2, far, spans, half, high, LAT), bf16),
            pltpu.VMEM((spans, C * blk, width), bf16),
            pltpu.VMEM((LAT // 128, N * stride, 128), jnp.float32),
            pltpu.VMEM((spans, C * slots, high, LAT), bf16),
            pltpu.SemaphoreType.REGULAR((2, far)), dma((4,)), dma((1,)), dma((2, far)),
            dma((1,)), dma((A,)), dma((max(S - 1, 1),)), dma((max(S - 1, 1),)),
            dma((1,)), dma((max(Y, 1),)),
            dma((1,)), dma((2, far)), dma((1,)), dma((2, far, max(S - 1, 1))),
            dma((1,)), dma((max(Z, 1),)),
        ],
        compiler_params=pltpu.CompilerParams(
            collective_id=0, has_side_effects=True, vmem_limit_bytes=48 * 1024 * 1024
        ),
    )(*(pltpu.with_memory_space_constraint(a, pltpu.HBM) for a in given))
    out = pl.pallas_call(
        functools.partial(finish, stride),
        out_shape=jax.ShapeDtypeStruct((N, hh, V), bf16),
        in_specs=[vmem],
        out_specs=vmem,
        compiler_params=pltpu.CompilerParams(vmem_limit_bytes=8 * 1024 * 1024),
    )(res)
    return out.reshape(spans, per_span, hh, V)


def solution(mesh):
    placed = (
        P(("groups", "ctx"), None, ("wt", "sub"), None),
        P(("groups", "ctx"), None, None),
        P(("groups", "ctx"), None, None),
        P(None, ("wt", "sub"), None),
    )
    return jax.shard_map(
        per_device,
        mesh=mesh,
        in_specs=placed,
        out_specs=P(("groups", "ctx"), None, ("wt", "sub"), None),
        check_vma=False,
    )
```

```python
import functools
import itertools

import jax
import jax.numpy as jnp
from jax import lax
from jax.experimental import pallas as pl
from jax.experimental.pallas import tpu as pltpu
from jax.sharding import PartitionSpec as P

LAT = 512
ROPE = 64
NOPE = 128
MESH = pl.DeviceIdType.MESH
T_K0, T_K1, T_F, T_P = 15.0, 5.4, 1.0, 18


def kernel(
    dims, sel_hbm, q_hbm, cache_hbm, up_hbm, res_v,
    q_v, cache_v, up_v, sel_sm, chosen, sel_far, send_v, keys_v, lat_v, kbuf,
    known, loc_sem, sel_snd, sel_rcv, x_snd, x_rcv, s_snd, s_rcv, y_snd, y_rcv,
    k_snd, k_rcv, f_snd, f_rcv, z_snd, z_rcv,
):
    (G, C, W, S, spans, per_span, hh, slots, blk, width, R, V, stride, A, Y, Z) = dims
    half = slots // S
    groups = LAT // ROPE
    RX = (W - 1) * S
    rows = per_span * hh
    N = spans * per_span
    n0 = max(hh - 2 * A, 0)
    g, c, w, s = (lax.axis_index(a) for a in ("groups", "ctx", "wt", "sub"))
    me = w * S + s
    odd = lax.rem(c, 2)
    base = g * A if Y else 0
    other = (G - 1 - g) * A if Y else 0

    def head(p):
        return p + odd * (hh - 1 - 2 * p) if Z else p

    def rowsof(k):
        return pl.ds(pl.multiple_of(k * R, R), R)

    def shift(i, d, n):
        return lax.rem(i + d + n, n)

    def inside(p):
        return jnp.logical_and(p >= 0, p < C)

    def both(a, b):
        return jnp.logical_and(a, b)

    locals_ = [
        pltpu.make_async_copy(sel_hbm, sel_sm, loc_sem.at[0]),
        pltpu.make_async_copy(cache_hbm, cache_v, loc_sem.at[1]),
        pltpu.make_async_copy(q_hbm, q_v, loc_sem.at[2]),
        pltpu.make_async_copy(
            up_hbm.at[pl.ds(pl.multiple_of(me * hh, hh), hh)], up_v.at[:, rowsof(me)], loc_sem.at[3]
        ),
    ]
    for copy in locals_:
        copy.start()

    barrier = pltpu.get_barrier_semaphore()
    for dw in range(W):
        for ds in range(S):
            if dw or ds:
                pl.semaphore_signal(
                    barrier, inc=1, device_id={"wt": shift(w, dw, W), "sub": shift(s, ds, S)},
                    device_id_type=MESH,
                )
    for dg in range(1, G):
        pl.semaphore_signal(barrier, inc=1, device_id={"groups": shift(g, dg, G)}, device_id_type=MESH)
    for step in (-1, 1):
        @pl.when(inside(c + step))
        def _():
            pl.semaphore_signal(barrier, inc=1, device_id={"ctx": c + step}, device_id_type=MESH)
    beside = (c > 0).astype(jnp.int32) + (c < C - 1).astype(jnp.int32)
    pl.semaphore_wait(barrier, W * S - 1 + G - 1 + beside)

    def x_copy(r, j, sending):
        dw, ds = r // S + 1, r % S
        if sending:
            w2, s2 = shift(w, dw, W), shift(s, ds, S)
            src_k, dst_k = me, w2 * S + s2
        else:
            w2, s2 = shift(w, -dw, W), shift(s, -ds, S)
            src_k, dst_k = w2 * S + s2, me
        h = head(base + j)
        return pltpu.make_async_remote_copy(
            up_hbm.at[dst_k * hh + h], up_v.at[h, rowsof(src_k)],
            x_snd.at[0], x_rcv.at[j],
            device_id={"wt": w2, "sub": s2}, device_id_type=MESH,
        )

    def far_rows(r):
        dw, ds = r // S + 1, r % S
        return rowsof(shift(w, -dw, W) * S + shift(s, -ds, S))

    def s_copy(ds, sending):
        s2 = shift(s, ds if sending else -ds, S)
        src_s, dst_s = (s, s2) if sending else (s2, s)
        start = pl.multiple_of((w * S + dst_s) * hh, hh)
        return pltpu.make_async_remote_copy(
            up_hbm.at[pl.ds(start, hh)], up_v.at[:, rowsof(w * S + src_s)],
            s_snd.at[ds - 1], s_rcv.at[ds - 1], device_id={"sub": s2}, device_id_type=MESH,
        )

    def y_copy(r, j, sending):
        region = up_v.at[head((base if sending else other) + j), far_rows(r)]
        return pltpu.make_async_remote_copy(
            region, region, y_snd.at[0], y_rcv.at[j],
            device_id={"groups": G - 1 - g}, device_id_type=MESH,
        )

    def z_from(j):
        return j if j < n0 else j + g * A

    def z_copy(r, j, sending):
        p = z_from(j)
        region = up_v.at[head(p if sending else hh - 1 - p), far_rows(r)]
        return pltpu.make_async_remote_copy(
            region, region, z_snd.at[0], z_rcv.at[j],
            device_id={"ctx": c + 1 - 2 * odd}, device_id_type=MESH,
        )

    def step_of(way):
        return 2 * way - 1

    def sel_copy(way, d):
        return pltpu.make_async_remote_copy(
            sel_hbm, sel_far.at[way, d - 1], sel_snd.at[0], sel_rcv.at[way, d - 1],
            device_id={"ctx": c + d * step_of(way)}, device_id_type=MESH,
        )

    def announce(d):
        for way in (1, 0):
            @pl.when(inside(c - d * step_of(way)))
            def _():
                if d > 1:
                    pl.semaphore_wait(known.at[way, d - 1], 1)
                if d < C - 1:
                    @pl.when(inside(c + step_of(way)))
                    def _():
                        pl.semaphore_signal(
                            known.at[way, d], inc=1, device_id={"ctx": c + step_of(way)}, device_id_type=MESH
                        )
                sel_copy(1 - way, d).start()

    def k_copy(way, d, sending):
        p = c + d * step_of(way) * (1 if sending else -1)
        first = (c if sending else p) * slots + s * half
        return pltpu.make_async_remote_copy(
            send_v.at[way, d - 1], kbuf.at[:, pl.ds(first, half)],
            k_snd.at[0], k_rcv.at[way, d - 1], device_id={"ctx": p}, device_id_type=MESH,
        )

    def f_copy(way, d, ds, sending):
        owner = c - d * step_of(way)
        s2 = shift(s, ds if sending else -ds, S)
        region = kbuf.at[:, pl.ds(owner * slots + (s if sending else s2) * half, half)]
        return pltpu.make_async_remote_copy(
            region, region, f_snd.at[0], f_rcv.at[way, d - 1, ds - 1],
            device_id={"sub": s2}, device_id_type=MESH,
        )

    def drain(region, sem):
        pltpu.make_async_copy(region, region, sem).wait()

    def unit_bytes(n):
        return up_v.at[pl.ds(0, n), pl.ds(0, RX * R)]

    if C > 1:
        announce(1)
    for j in range(A):
        for r in range(RX):
            x_copy(r, j, True).start()
    for d in range(2, C):
        announce(d)
    for ds in range(1, S):
        s_copy(ds, True).start()

    last = cache_v.shape[0] - 1

    tall = blk // groups

    def pack(dst, entry):
        n = jnp.clip(entry, 0, last)
        dst[:blk, :] = cache_v[n, :, :LAT]
        dst[blk:, :] = jnp.concatenate(
            [cache_v[n, q * tall : (q + 1) * tall, LAT:] for q in range(groups)], axis=1
        )

    def round_(d):
        for way in (1, 0):
            @pl.when(inside(c - d * step_of(way)))
            def _():
                sel_copy(way, d).wait_recv()
                for i in range(spans):
                    for t in range(half):
                        pack(send_v.at[1 - way, d - 1, i, t], sel_far[way, d - 1, i, s * half + t, c])
                k_copy(1 - way, d, True).start()

    def x_recv(j):
        drain(unit_bytes(1), x_rcv.at[j])
        for r in range(RX if j < Y else 0):
            y_copy(r, j, True).start()

    def x_pass(j):
        for r in range(RX):
            if j >= n0:
                z_copy(r, j, True).start()
            else:
                pl.when(g == 0)(z_copy(r, j, True).start)

    def y_recv(j):
        drain(unit_bytes(1), y_rcv.at[j])

    def y_pass(j):
        @pl.when(g > 0)
        def _():
            y_recv(j)
            for r in range(RX):
                z_copy(r, j, True).start()

    def y_late(j):
        pl.when(g == 0)(lambda: y_recv(j))

    def z_recv(j):
        drain(unit_bytes(1), z_rcv.at[j])

    def k_recv(d):
        for way in range(2):
            @pl.when(inside(c - d * step_of(way)))
            def _():
                k_copy(way, d, False).wait_recv()
                for ds in range(1, S):
                    f_copy(way, d, ds, True).start()

    scale = jnp.float32((NOPE + ROPE) ** (-0.5))
    share = min(32, per_span)
    tile = share * hh

    def live_slots(i):
        total = C * slots

        def find(n, carry):
            rank, picks = carry
            live = sel_sm[i, lax.rem(n, slots), n // slots] >= 0
            picks = tuple(
                jnp.where(both(live, rank == at), n, old) for at, old in enumerate(picks)
            )
            return rank + live.astype(jnp.int32), picks

        zero = jnp.int32(0)
        return lax.fori_loop(0, total, find, (zero, (zero,) * C))[1]

    def gathered():
        for d in range(1, C):
            for way in range(2):
                for ds in range(1, S):
                    pl.when(inside(c - d * step_of(way)))(f_copy(way, d, ds, False).wait_recv)

    def collect(i):
        for at in range(C):
            slot = chosen[i, at]
            keys_v[i, at * blk : (at + 1) * blk, :LAT] = kbuf[i, slot, :blk, :]
            for q in range(groups):
                low = at * blk + q * tall
                keys_v[i, low : low + tall, LAT:] = kbuf[i, slot, blk:, q * ROPE : (q + 1) * ROPE]

    def attend():
        for i, at in itertools.product(range(spans), range(per_span // share)):
            top = i * rows + at * tile
            keys = keys_v[i]
            scores = lax.dot_general(
                q_v[top : top + tile, :], keys, (((1,), (1,)), ((), ())),
                preferred_element_type=jnp.float32,
            ) * scale
            expo = jnp.exp(scores - jnp.max(scores, axis=1, keepdims=True))
            totals = jnp.sum(expo, axis=1, keepdims=True)
            latent = jnp.dot(
                expo.astype(jnp.bfloat16), keys[:, :LAT], preferred_element_type=jnp.float32
            ) / totals
            for l in range(LAT // 128):
                for n in range(share):
                    at_row = (i * per_span + at * share + n) * stride
                    lat_v[l, at_row : at_row + hh, :] = latent[n * hh : (n + 1) * hh, l * 128 : (l + 1) * 128]

    def project(heads):
        for h in heads:
            left = jnp.concatenate(
                [lat_v[l, pl.ds(h, N, stride=stride), :].astype(jnp.bfloat16) for l in range(LAT // 128)],
                axis=1,
            )
            res_v[pl.ds(h, N, stride=stride), :] = jnp.dot(
                left, up_v[h], preferred_element_type=jnp.float32
            )

    def prepare():
        locals_[0].wait()
        for i in range(spans):
            for t in range(slots):
                pack(kbuf.at[i, c * slots + t], sel_sm[i, t, c])
            for at, slot in enumerate(live_slots(i)):
                chosen[i, at] = slot
        locals_[2].wait()

    def ready():
        locals_[3].wait()
        for ds in range(1, S):
            s_copy(ds, False).wait_recv()

    events = []

    def at(time, act, *args):
        events.append((time, len(events), act, args))

    unit, lead = 1.43 * 32 / hh, 7.0
    keys_at = [T_K0 + T_K1 * (d + 1) / (C - 1) for d in range(C - 1)]
    start = keys_at[-1] + T_F if C > 1 else lead
    done = start + 1.3 * spans
    locals_[1].wait()
    for d in range(1, C):
        at(lead + (1.0 * d - 2.0 if C < 8 else 0.0), round_, d)
        at(keys_at[d - 1], k_recv, d)
    at(lead + 0.5, prepare)
    at(start, gathered)
    for i in range(spans):
        at(start, collect, i)
    at(start, attend)
    at(done, ready)
    for j in range(A):
        x_at = lead + unit * j
        at(x_at, x_recv, j)
        if j < Z:
            at(max(x_at, lead + 2.0), x_pass, j)
        at(max(x_at, done), project, head(base + j))
        if j < Y:
            y_at = x_at + 3.5
            if j < min(n0, Z):
                at(y_at + 1.0, y_pass, j)
                at(max(y_at, done), y_late, j)
            else:
                at(max(y_at, done), y_recv, j)
            at(max(y_at, done), project, head(other + j))
    for j in range(Z):
        z_at = max(lead + unit * (A - 1 - (Z - 1 - j)), done)
        at(z_at, z_recv, j)
        at(z_at, project, head(hh - 1 - z_from(j)))
    events.sort(key=lambda e: e[:2])
    heads = []
    for _, _, act, args in events:
        if act is project:
            heads.extend(args)
            if len(heads) < T_P:
                continue
        if act is project:
            project(heads)
            heads = []
        else:
            act(*args)
    project(heads)

    if C > 1:
        drain(sel_far.at[0], sel_snd.at[0])
        drain(send_v.at[0], k_snd.at[0])
        if S > 1:
            drain(send_v.at[pl.ds(0, S - 1)], f_snd.at[0])
    for ds in range(1, S):
        s_copy(ds, True).wait_send()
    if RX:
        for count, sem in ((A, x_snd), (Y, y_snd), (Z, z_snd)):
            if count:
                drain(unit_bytes(count), sem.at[0])


def finish(stride, res_ref, out_ref):
    hh = out_ref.shape[1]

    for n in range(out_ref.shape[0]):
        out_ref[n] = res_ref[n * stride : n * stride + hh, :].astype(jnp.bfloat16)


def split(G, C, hh):
    if G != 2 or C % 2 or hh < 8:
        return hh, 0, 0
    A = (15 * hh) // 32
    Y = (11 * hh) // 32
    return A, Y, hh - A - Y


def per_device(queries, selection, latent_cache, value_up):
    G, C, W, S = (lax.axis_size(a) for a in ("groups", "ctx", "wt", "sub"))
    spans, per_span, hh, width = queries.shape
    slots = selection.shape[2]
    blk = latent_cache.shape[1]
    R, V = value_up.shape[1:]
    A, Y, Z = split(G, C, hh)
    stride = hh + 8
    N = spans * per_span
    RX = (W - 1) * S
    half = slots // S
    high = blk + blk * ROPE // LAT
    far = max(C - 1, 1)
    dims = (G, C, W, S, spans, per_span, hh, slots, blk, width, R, V, stride, A, Y, Z)
    bf16, dma = jnp.bfloat16, pltpu.SemaphoreType.DMA
    hbm = pl.BlockSpec(memory_space=pltpu.HBM)
    vmem = pl.BlockSpec(memory_space=pltpu.VMEM)
    given = (selection.transpose(0, 2, 1), queries.reshape(N * hh, width), latent_cache, value_up)
    res = pl.pallas_call(
        functools.partial(kernel, dims),
        out_shape=pltpu.VMEM((N * stride, V), jnp.float32),
        in_specs=[hbm] * 4,
        out_specs=vmem,
        scratch_shapes=[
            pltpu.VMEM((N * hh, width), bf16),
            pltpu.VMEM(latent_cache.shape, bf16),
            pltpu.VMEM((hh, LAT, V), bf16),
            pltpu.SMEM((spans, slots, C), jnp.int32),
            pltpu.SMEM((spans, C), jnp.int32),
            pltpu.SMEM((2, far, spans, slots, C), jnp.int32),
            pltpu.VMEM((2, far, spans, half, high, LAT), bf16),
            pltpu.VMEM((spans, C * blk, width), bf16),
            pltpu.VMEM((LAT // 128, N * stride, 128), jnp.float32),
            pltpu.VMEM((spans, C * slots, high, LAT), bf16),
            pltpu.SemaphoreType.REGULAR((2, far)), dma((4,)), dma((1,)), dma((2, far)),
            dma((1,)), dma((A,)), dma((max(S - 1, 1),)), dma((max(S - 1, 1),)),
            dma((1,)), dma((max(Y, 1),)),
            dma((1,)), dma((2, far)), dma((1,)), dma((2, far, max(S - 1, 1))),
            dma((1,)), dma((max(Z, 1),)),
        ],
        compiler_params=pltpu.CompilerParams(
            collective_id=0, has_side_effects=True, vmem_limit_bytes=48 * 1024 * 1024
        ),
    )(*(pltpu.with_memory_space_constraint(a, pltpu.HBM) for a in given))
    out = pl.pallas_call(
        functools.partial(finish, stride),
        out_shape=jax.ShapeDtypeStruct((N, hh, V), bf16),
        in_specs=[vmem],
        out_specs=vmem,
        compiler_params=pltpu.CompilerParams(vmem_limit_bytes=8 * 1024 * 1024),
    )(res)
    return out.reshape(spans, per_span, hh, V)


def solution(mesh):
    placed = (
        P(("groups", "ctx"), None, ("wt", "sub"), None),
        P(("groups", "ctx"), None, None),
        P(("groups", "ctx"), None, None),
        P(None, ("wt", "sub"), None),
    )
    return jax.shard_map(
        per_device,
        mesh=mesh,
        in_specs=placed,
        out_specs=P(("groups", "ctx"), None, ("wt", "sub"), None),
        check_vma=False,
    )
```

```python
import functools
import itertools

import jax
import jax.numpy as jnp
from jax import lax
from jax.experimental import pallas as pl
from jax.experimental.pallas import tpu as pltpu
from jax.sharding import PartitionSpec as P

LAT = 512
ROPE = 64
NOPE = 128
MESH = pl.DeviceIdType.MESH
T_K0, T_K1, T_F, T_P = 19.2, 1.2, 1.0, 26


def kernel(
    dims, sel_hbm, q_hbm, cache_hbm, up_hbm, res_v,
    q_v, cache_v, up_v, sel_sm, chosen, sel_far, send_v, keys_v, lat_v, kbuf,
    known, loc_sem, sel_snd, sel_rcv, x_snd, x_rcv, s_snd, s_rcv, y_snd, y_rcv,
    k_snd, k_rcv, f_snd, f_rcv, z_snd, z_rcv,
):
    (G, C, W, S, spans, per_span, hh, slots, blk, width, R, V, stride, A, Y, Z) = dims
    half = slots // S
    groups = LAT // ROPE
    RX = (W - 1) * S
    rows = per_span * hh
    N = spans * per_span
    n0 = max(hh - 2 * A, 0)
    g, c, w, s = (lax.axis_index(a) for a in ("groups", "ctx", "wt", "sub"))
    me = w * S + s
    odd = lax.rem(c, 2)
    base = g * A if Y else 0
    other = (G - 1 - g) * A if Y else 0

    def head(p):
        return p + odd * (hh - 1 - 2 * p) if Z else p

    def rowsof(k):
        return pl.ds(pl.multiple_of(k * R, R), R)

    def shift(i, d, n):
        return lax.rem(i + d + n, n)

    def inside(p):
        return jnp.logical_and(p >= 0, p < C)

    def both(a, b):
        return jnp.logical_and(a, b)

    locals_ = [
        pltpu.make_async_copy(sel_hbm, sel_sm, loc_sem.at[0]),
        pltpu.make_async_copy(cache_hbm, cache_v, loc_sem.at[1]),
        pltpu.make_async_copy(q_hbm, q_v, loc_sem.at[2]),
        pltpu.make_async_copy(
            up_hbm.at[pl.ds(pl.multiple_of(me * hh, hh), hh)], up_v.at[:, rowsof(me)], loc_sem.at[3]
        ),
    ]
    for copy in locals_:
        copy.start()

    barrier = pltpu.get_barrier_semaphore()
    for dw in range(W):
        for ds in range(S):
            if dw or ds:
                pl.semaphore_signal(
                    barrier, inc=1, device_id={"wt": shift(w, dw, W), "sub": shift(s, ds, S)},
                    device_id_type=MESH,
                )
    for dg in range(1, G):
        pl.semaphore_signal(barrier, inc=1, device_id={"groups": shift(g, dg, G)}, device_id_type=MESH)
    for step in (-1, 1):
        @pl.when(inside(c + step))
        def _():
            pl.semaphore_signal(barrier, inc=1, device_id={"ctx": c + step}, device_id_type=MESH)
    beside = (c > 0).astype(jnp.int32) + (c < C - 1).astype(jnp.int32)
    pl.semaphore_wait(barrier, W * S - 1 + G - 1 + beside)

    def x_copy(r, j, sending):
        dw, ds = r // S + 1, r % S
        if sending:
            w2, s2 = shift(w, dw, W), shift(s, ds, S)
            src_k, dst_k = me, w2 * S + s2
        else:
            w2, s2 = shift(w, -dw, W), shift(s, -ds, S)
            src_k, dst_k = w2 * S + s2, me
        h = head(base + j)
        return pltpu.make_async_remote_copy(
            up_hbm.at[dst_k * hh + h], up_v.at[h, rowsof(src_k)],
            x_snd.at[0], x_rcv.at[j],
            device_id={"wt": w2, "sub": s2}, device_id_type=MESH,
        )

    def far_rows(r):
        dw, ds = r // S + 1, r % S
        return rowsof(shift(w, -dw, W) * S + shift(s, -ds, S))

    def s_copy(ds, sending):
        s2 = shift(s, ds if sending else -ds, S)
        src_s, dst_s = (s, s2) if sending else (s2, s)
        start = pl.multiple_of((w * S + dst_s) * hh, hh)
        return pltpu.make_async_remote_copy(
            up_hbm.at[pl.ds(start, hh)], up_v.at[:, rowsof(w * S + src_s)],
            s_snd.at[ds - 1], s_rcv.at[ds - 1], device_id={"sub": s2}, device_id_type=MESH,
        )

    def y_copy(r, j, sending):
        region = up_v.at[head((base if sending else other) + j), far_rows(r)]
        return pltpu.make_async_remote_copy(
            region, region, y_snd.at[0], y_rcv.at[j],
            device_id={"groups": G - 1 - g}, device_id_type=MESH,
        )

    def z_from(j):
        return j if j < n0 else j + g * A

    def z_copy(r, j, sending):
        p = z_from(j)
        region = up_v.at[head(p if sending else hh - 1 - p), far_rows(r)]
        return pltpu.make_async_remote_copy(
            region, region, z_snd.at[0], z_rcv.at[j],
            device_id={"ctx": c + 1 - 2 * odd}, device_id_type=MESH,
        )

    def step_of(way):
        return 2 * way - 1

    def sel_copy(way, d):
        return pltpu.make_async_remote_copy(
            sel_hbm, sel_far.at[way, d - 1], sel_snd.at[0], sel_rcv.at[way, d - 1],
            device_id={"ctx": c + d * step_of(way)}, device_id_type=MESH,
        )

    def announce(d):
        for way in (1, 0):
            @pl.when(inside(c - d * step_of(way)))
            def _():
                if d > 1:
                    pl.semaphore_wait(known.at[way, d - 1], 1)
                if d < C - 1:
                    @pl.when(inside(c + step_of(way)))
                    def _():
                        pl.semaphore_signal(
                            known.at[way, d], inc=1, device_id={"ctx": c + step_of(way)}, device_id_type=MESH
                        )
                sel_copy(1 - way, d).start()

    def k_copy(way, d, sending):
        p = c + d * step_of(way) * (1 if sending else -1)
        first = (c if sending else p) * slots + s * half
        return pltpu.make_async_remote_copy(
            send_v.at[way, d - 1], kbuf.at[:, pl.ds(first, half)],
            k_snd.at[0], k_rcv.at[way, d - 1], device_id={"ctx": p}, device_id_type=MESH,
        )

    def f_copy(way, d, ds, sending):
        owner = c - d * step_of(way)
        s2 = shift(s, ds if sending else -ds, S)
        region = kbuf.at[:, pl.ds(owner * slots + (s if sending else s2) * half, half)]
        return pltpu.make_async_remote_copy(
            region, region, f_snd.at[0], f_rcv.at[way, d - 1, ds - 1],
            device_id={"sub": s2}, device_id_type=MESH,
        )

    def drain(region, sem):
        pltpu.make_async_copy(region, region, sem).wait()

    def unit_bytes(n):
        return up_v.at[pl.ds(0, n), pl.ds(0, RX * R)]

    if C > 1:
        announce(1)
    for j in range(A):
        for r in range(RX):
            x_copy(r, j, True).start()
    for d in range(2, C):
        announce(d)
    for ds in range(1, S):
        s_copy(ds, True).start()

    last = cache_v.shape[0] - 1

    tall = blk // groups

    def pack(dst, entry):
        n = jnp.clip(entry, 0, last)
        dst[:blk, :] = cache_v[n, :, :LAT]
        dst[blk:, :] = jnp.concatenate(
            [cache_v[n, q * tall : (q + 1) * tall, LAT:] for q in range(groups)], axis=1
        )

    def round_(d):
        for way in (1, 0):
            @pl.when(inside(c - d * step_of(way)))
            def _():
                sel_copy(way, d).wait_recv()
                for i in range(spans):
                    for t in range(half):
                        pack(send_v.at[1 - way, d - 1, i, t], sel_far[way, d - 1, i, s * half + t, c])
                k_copy(1 - way, d, True).start()

    def x_recv(j):
        drain(unit_bytes(1), x_rcv.at[j])
        for r in range(RX if j < Y else 0):
            y_copy(r, j, True).start()

    def x_pass(j):
        for r in range(RX):
            if j >= n0:
                z_copy(r, j, True).start()
            else:
                pl.when(g == 0)(z_copy(r, j, True).start)

    def y_recv(j):
        drain(unit_bytes(1), y_rcv.at[j])

    def y_pass(j):
        @pl.when(g > 0)
        def _():
            y_recv(j)
            for r in range(RX):
                z_copy(r, j, True).start()

    def y_late(j):
        pl.when(g == 0)(lambda: y_recv(j))

    def z_recv(j):
        drain(unit_bytes(1), z_rcv.at[j])

    def k_recv(d):
        for way in range(2):
            @pl.when(inside(c - d * step_of(way)))
            def _():
                k_copy(way, d, False).wait_recv()
                for ds in range(1, S):
                    f_copy(way, d, ds, True).start()

    scale = jnp.float32((NOPE + ROPE) ** (-0.5))
    share = min(32, per_span)
    tile = share * hh

    def live_slots(i):
        total = C * slots

        def find(n, carry):
            rank, picks = carry
            live = sel_sm[i, lax.rem(n, slots), n // slots] >= 0
            picks = tuple(
                jnp.where(both(live, rank == at), n, old) for at, old in enumerate(picks)
            )
            return rank + live.astype(jnp.int32), picks

        zero = jnp.int32(0)
        return lax.fori_loop(0, total, find, (zero, (zero,) * C))[1]

    def gathered():
        for d in range(1, C):
            for way in range(2):
                for ds in range(1, S):
                    pl.when(inside(c - d * step_of(way)))(f_copy(way, d, ds, False).wait_recv)

    def collect(i):
        for at in range(C):
            slot = chosen[i, at]
            keys_v[i, at * blk : (at + 1) * blk, :LAT] = kbuf[i, slot, :blk, :]
            for q in range(groups):
                low = at * blk + q * tall
                keys_v[i, low : low + tall, LAT:] = kbuf[i, slot, blk:, q * ROPE : (q + 1) * ROPE]

    def attend():
        for i, at in itertools.product(range(spans), range(per_span // share)):
            top = i * rows + at * tile
            keys = keys_v[i]
            scores = lax.dot_general(
                q_v[top : top + tile, :], keys, (((1,), (1,)), ((), ())),
                preferred_element_type=jnp.float32,
            ) * scale
            expo = jnp.exp(scores - jnp.max(scores, axis=1, keepdims=True))
            totals = jnp.sum(expo, axis=1, keepdims=True)
            latent = jnp.dot(
                expo.astype(jnp.bfloat16), keys[:, :LAT], preferred_element_type=jnp.float32
            ) / totals
            for l in range(LAT // 128):
                for n in range(share):
                    at_row = (i * per_span + at * share + n) * stride
                    lat_v[l, at_row : at_row + hh, :] = latent[n * hh : (n + 1) * hh, l * 128 : (l + 1) * 128]

    def project(heads):
        for h in heads:
            left = jnp.concatenate(
                [lat_v[l, pl.ds(h, N, stride=stride), :].astype(jnp.bfloat16) for l in range(LAT // 128)],
                axis=1,
            )
            res_v[pl.ds(h, N, stride=stride), :] = jnp.dot(
                left, up_v[h], preferred_element_type=jnp.float32
            )

    def prepare():
        locals_[0].wait()
        for i in range(spans):
            for t in range(slots):
                pack(kbuf.at[i, c * slots + t], sel_sm[i, t, c])
            for at, slot in enumerate(live_slots(i)):
                chosen[i, at] = slot
        locals_[2].wait()

    def ready():
        locals_[3].wait()
        for ds in range(1, S):
            s_copy(ds, False).wait_recv()

    events = []

    def at(time, act, *args):
        events.append((time, len(events), act, args))

    unit, lead = 1.43 * 32 / hh, 7.0
    keys_at = [T_K0 + T_K1 * (d + 1) / (C - 1) for d in range(C - 1)]
    start = keys_at[-1] + T_F if C > 1 else lead
    done = start + 1.3 * spans
    locals_[1].wait()
    for d in range(1, C):
        at(lead + (1.0 * d - 2.0 if C < 8 else 0.0), round_, d)
        at(keys_at[d - 1], k_recv, d)
    at(lead + 3.5, prepare)
    at(start, gathered)
    for i in range(spans):
        at(start, collect, i)
    at(start, attend)
    at(done, ready)
    for j in range(A):
        x_at = lead + unit * j
        at(x_at, x_recv, j)
        if j < Z:
            at(max(x_at, lead + 2.0), x_pass, j)
        at(max(x_at, done), project, head(base + j))
        if j < Y:
            y_at = x_at + 3.5
            if j < min(n0, Z):
                at(y_at + 1.0, y_pass, j)
                at(max(y_at, done), y_late, j)
            else:
                at(max(y_at, done), y_recv, j)
            at(max(y_at, done), project, head(other + j))
    for j in range(Z):
        z_at = max(lead + unit * (A - 1 - (Z - 1 - j)), done)
        at(z_at, z_recv, j)
        at(z_at, project, head(hh - 1 - z_from(j)))
    events.sort(key=lambda e: e[:2])
    heads = []
    for _, _, act, args in events:
        if act is project:
            heads.extend(args)
            if len(heads) < T_P:
                continue
        if act is project:
            project(heads)
            heads = []
        else:
            act(*args)
    project(heads)

    if C > 1:
        drain(sel_far.at[0], sel_snd.at[0])
        drain(send_v.at[0], k_snd.at[0])
        if S > 1:
            drain(send_v.at[pl.ds(0, S - 1)], f_snd.at[0])
    for ds in range(1, S):
        s_copy(ds, True).wait_send()
    if RX:
        for count, sem in ((A, x_snd), (Y, y_snd), (Z, z_snd)):
            if count:
                drain(unit_bytes(count), sem.at[0])


def finish(stride, res_ref, out_ref):
    hh = out_ref.shape[1]

    for n in range(out_ref.shape[0]):
        out_ref[n] = res_ref[n * stride : n * stride + hh, :].astype(jnp.bfloat16)


def split(G, C, hh):
    if G != 2 or C % 2 or hh < 8:
        return hh, 0, 0
    A = (15 * hh) // 32
    Y = (11 * hh) // 32
    return A, Y, hh - A - Y


def per_device(queries, selection, latent_cache, value_up):
    G, C, W, S = (lax.axis_size(a) for a in ("groups", "ctx", "wt", "sub"))
    spans, per_span, hh, width = queries.shape
    slots = selection.shape[2]
    blk = latent_cache.shape[1]
    R, V = value_up.shape[1:]
    A, Y, Z = split(G, C, hh)
    stride = hh + 8
    N = spans * per_span
    RX = (W - 1) * S
    half = slots // S
    high = blk + blk * ROPE // LAT
    far = max(C - 1, 1)
    dims = (G, C, W, S, spans, per_span, hh, slots, blk, width, R, V, stride, A, Y, Z)
    bf16, dma = jnp.bfloat16, pltpu.SemaphoreType.DMA
    hbm = pl.BlockSpec(memory_space=pltpu.HBM)
    vmem = pl.BlockSpec(memory_space=pltpu.VMEM)
    given = (selection.transpose(0, 2, 1), queries.reshape(N * hh, width), latent_cache, value_up)
    res = pl.pallas_call(
        functools.partial(kernel, dims),
        out_shape=pltpu.VMEM((N * stride, V), jnp.float32),
        in_specs=[hbm] * 4,
        out_specs=vmem,
        scratch_shapes=[
            pltpu.VMEM((N * hh, width), bf16),
            pltpu.VMEM(latent_cache.shape, bf16),
            pltpu.VMEM((hh, LAT, V), bf16),
            pltpu.SMEM((spans, slots, C), jnp.int32),
            pltpu.SMEM((spans, C), jnp.int32),
            pltpu.SMEM((2, far, spans, slots, C), jnp.int32),
            pltpu.VMEM((2, far, spans, half, high, LAT), bf16),
            pltpu.VMEM((spans, C * blk, width), bf16),
            pltpu.VMEM((LAT // 128, N * stride, 128), jnp.float32),
            pltpu.VMEM((spans, C * slots, high, LAT), bf16),
            pltpu.SemaphoreType.REGULAR((2, far)), dma((4,)), dma((1,)), dma((2, far)),
            dma((1,)), dma((A,)), dma((max(S - 1, 1),)), dma((max(S - 1, 1),)),
            dma((1,)), dma((max(Y, 1),)),
            dma((1,)), dma((2, far)), dma((1,)), dma((2, far, max(S - 1, 1))),
            dma((1,)), dma((max(Z, 1),)),
        ],
        compiler_params=pltpu.CompilerParams(
            collective_id=0, has_side_effects=True, vmem_limit_bytes=48 * 1024 * 1024
        ),
    )(*(pltpu.with_memory_space_constraint(a, pltpu.HBM) for a in given))
    out = pl.pallas_call(
        functools.partial(finish, stride),
        out_shape=jax.ShapeDtypeStruct((N, hh, V), bf16),
        in_specs=[vmem],
        out_specs=vmem,
        compiler_params=pltpu.CompilerParams(vmem_limit_bytes=8 * 1024 * 1024),
    )(res)
    return out.reshape(spans, per_span, hh, V)


def solution(mesh):
    placed = (
        P(("groups", "ctx"), None, ("wt", "sub"), None),
        P(("groups", "ctx"), None, None),
        P(("groups", "ctx"), None, None),
        P(None, ("wt", "sub"), None),
    )
    return jax.shard_map(
        per_device,
        mesh=mesh,
        in_specs=placed,
        out_specs=P(("groups", "ctx"), None, ("wt", "sub"), None),
        check_vma=False,
    )
```
